128 devices in a mesh: dev: 128 (over y, z, x, core).
Axes of the slice: x: 4, y: 4, z: 4, core: 2. Of those that a mesh axis runs over, the one named last changes fastest.
Arguments:
- state_real: float32 [16777216], P('dev'), may hold values from -24 to 24, as said below
- state_imag: float32 [16777216], P('dev'), may hold values from -24 to 24, as said below
- subsystem: int32 [3], replicated, may hold values from 0 to 16, as said below
Outputs:
- rho_real: float32 [1024, 1024], P('dev')
- rho_imag: float32 [1024, 1024], P('dev')
The draws below stay inside these ranges and needn't reach their ends.
Inputs may be any that keep to these rules, and one draw needn't show every extreme that they name: `subsystem`: the 3 entries are distinct local bit positions in ascending order; the first is always 0 and the last always 17 - 1. `state_real`: real parts of amplitudes; their typical size changes between aligned blocks of 2**(11) local indices by up to a factor of 16. `state_imag`: imaginary parts of amplitudes, with the same block sizes as the real parts.
All inputs are finite; a program needn't handle non-finite values.
Results may differ from the reference program's by a relative error of at most 0.0001.
Values sent between devices are 32-bit elements; how exact they have to be, the bound alone decides.
No kernel may reach another device: no remote copies, remote signals or barrier semaphores. Data moves between devices by JAX's collectives and lax.ppermute only.
A program may use at most 192 MiB of HBM per device.

```python
import jax
import jax.numpy as jnp
from jax import lax

LOCAL_QUBITS = 17
SUB_LOCAL = 3
AMPS_DEV = 131072
AMPS = 16777216
COMPLEMENT = 16384
SUB_DIM = 1024
N_DEV = 128


def amplitude_envelope(key):
    block_total = AMPS // 2 ** (LOCAL_QUBITS - 6)
    levels = jax.random.uniform(jax.random.fold_in(key, 11), (block_total,), jnp.float32, -1.3862943611198906, 1.3862943611198906)
    return jnp.repeat(jnp.exp(levels), AMPS // block_total, total_repeat_length=AMPS)


def draw_noise(key, salt_value):
    noise_key = jax.random.fold_in(key, salt_value)
    return jnp.clip(jax.random.normal(noise_key, (AMPS,), jnp.float32), -6.0, 6.0)


def draw_state_real(key, part):
    return (amplitude_envelope(key) * draw_noise(key, 3)).astype(jnp.float32)


def draw_state_imag(key, part):
    return (amplitude_envelope(key) * draw_noise(key, 5)).astype(jnp.float32)


def draw_subsystem(key, part):
    middle = jax.random.randint(jax.random.fold_in(key, 17), (1,), 1, LOCAL_QUBITS - 1, jnp.int32)
    lowest = jnp.zeros((1,), jnp.int32)
    highest = jnp.full((1,), LOCAL_QUBITS - 1, jnp.int32)
    return jnp.concatenate([lowest, middle, highest]).astype(jnp.int32)


def setup_inputs(seed: int = 0) -> dict:
    arg_keys = jax.random.split(jax.random.key(seed), 4)
    state_real = draw_state_real(jax.random.fold_in(arg_keys[3], 71), 0)
    state_imag = draw_state_imag(jax.random.fold_in(arg_keys[3], 71), 0)
    subsystem = draw_subsystem(jax.random.fold_in(arg_keys[3], 71), 0)
    return dict(state_real=state_real, state_imag=state_imag, subsystem=subsystem)


def insert_bits(subsystem, count_sub, count_rest):
    picked = lax.broadcasted_iota(jnp.int32, (count_sub, count_rest), 0)
    source = lax.broadcasted_iota(jnp.int32, (count_sub, count_rest), 1)
    for sub_index in range(subsystem.shape[0]):
        bit_place = subsystem[sub_index].astype(jnp.int32)
        lower_bits = jnp.bitwise_and(source, jnp.left_shift(jnp.int32(1), bit_place) - jnp.int32(1))
        upper_bits = jnp.left_shift(jnp.right_shift(source, bit_place), bit_place + jnp.int32(1))
        chosen_bit = jnp.left_shift(jnp.bitwise_and(jnp.right_shift(picked, sub_index), jnp.int32(1)), bit_place)
        source = upper_bits + chosen_bit + lower_bits
    return source


def contract(left, right):
    return lax.dot_general(left, right, (((1,), (1,)), ((), ())), precision=lax.Precision.HIGHEST, preferred_element_type=jnp.float32)


def reference(state_real, state_imag, subsystem):
    source_map = insert_bits(subsystem, 2 ** SUB_LOCAL, COMPLEMENT)
    psi_real = state_real.reshape(N_DEV, AMPS_DEV)[:, source_map].reshape(SUB_DIM, COMPLEMENT)
    psi_imag = state_imag.reshape(N_DEV, AMPS_DEV)[:, source_map].reshape(SUB_DIM, COMPLEMENT)
    inverse_rest = 1.0 / COMPLEMENT
    rho_real = (contract(psi_real, psi_real) + contract(psi_imag, psi_imag)) * inverse_rest
    rho_imag = (contract(psi_imag, psi_real) - contract(psi_real, psi_imag)) * inverse_rest
    return rho_real, rho_imag
```

```python
import jax
import jax.numpy as jnp
from jax import lax
from jax.experimental import pallas as pl
from jax.experimental.pallas import tpu as pltpu
from jax.sharding import Mesh
from jax.sharding import PartitionSpec as P

DEV = ("yh", "yl", "zh", "zl", "xh", "xl", "c")
PEERS = ("yl", "zh", "zl", "xh", "xl")
LANES = 128
ROWS = 1024
PARTS = 8


def lane_source(middle, lane):
    low_top = lane >> 6
    rest6 = lane & 63
    plain = low_top | (rest6 << 1)
    m = jnp.clip(middle, 1, 6)
    rest5 = lane & 31
    below = rest5 & ((1 << (m - 1)) - 1)
    above = rest5 >> (m - 1)
    both = low_top | (below << 1) | (((lane >> 5) & 1) << m) | (above << (m + 1))
    return jnp.where(middle < 7, both, plain)


def sublane_source(middle, sub):
    m = jnp.clip(middle - 7, 0, 2)
    rest = sub & 3
    below = rest & ((1 << m) - 1)
    above = rest >> m
    return below | ((sub >> 2) << m) | (above << (m + 1))


def regroup_kernel(sub_ref, re_ref, im_ref, out_ref, buf, sems):
    middle = sub_ref[1]
    lane = lax.broadcasted_iota(jnp.int32, (8, LANES), 1)
    sub = lax.broadcasted_iota(jnp.int32, (8, LANES), 0)
    lane_index = lane_source(middle, lane)
    sub_index = sublane_source(middle, sub)
    low64 = lane < 64
    low32 = (lane & 32) == 0
    low4 = sub < 4

    def load(ref, tile):
        return ref[pl.ds(pl.multiple_of(tile * 8, 8), 8), :]

    def lanes(value):
        return jnp.take_along_axis(value, lane_index, axis=1)

    def swap64(a, b):
        return (
            jnp.where(low64, a, pltpu.roll(b, 64, 1)),
            jnp.where(low64, pltpu.roll(a, 64, 1), b),
        )

    def swap32(a, b):
        return (
            jnp.where(low32, a, pltpu.roll(b, 32, 1)),
            jnp.where(low32, pltpu.roll(a, 96, 1), b),
        )

    def swap_sub(a, b):
        return (
            jnp.where(low4, a, pltpu.roll(b, 4, 0)),
            jnp.where(low4, pltpu.roll(a, 4, 0), b),
        )

    def lane_case(ref, top, k4):
        base = top * 64 + k4 * 4
        a = [lanes(load(ref, base + r)) for r in range(4)]
        b00, b10 = swap64(a[0], a[2])
        b01, b11 = swap64(a[1], a[3])
        return (*swap32(b00, b01), *swap32(b10, b11))

    def sub_case(ref, top, k4):
        base = top * 64 + k4 * 4
        a = [jnp.take_along_axis(lanes(load(ref, base + r)), sub_index, axis=0) for r in range(4)]
        b00, b10 = swap64(a[0], a[2])
        b01, b11 = swap64(a[1], a[3])
        return (*swap_sub(b00, b01), *swap_sub(b10, b11))

    def tile_case(ref, top, k4):
        m = jnp.clip(middle - 10, 0, 5)
        out = []
        for bit in range(2):
            pair = []
            for r in range(2):
                rest = k4 * 2 + r
                below = rest & ((1 << m) - 1)
                above = rest >> m
                tile = top * 64 + (below | (bit << m) | (above << (m + 1)))
                pair.append(lanes(load(ref, tile)))
            out.append(swap64(*pair))
        return (out[0][0], out[1][0], out[0][1], out[1][1])

    def run(case):
        def step(k4, carry):
            for array, ref in enumerate((re_ref, im_ref)):
                for top in range(2):
                    tiles = case(ref, top, k4)
                    for which, tile in enumerate(tiles):
                        part = (which >> 1) + 2 * (which & 1) + 4 * top
                        row = (k4 >> 1) * 32 + array * 16 + (k4 & 1) * 8 + part
                        buf[pl.ds(row, 8, stride=256), :] = tile
            return carry

        lax.fori_loop(0, 16, step, 0)

    @pl.when(middle < 7)
    def _():
        run(lane_case)

    @pl.when((middle >= 7) & (middle < 10))
    def _():
        run(sub_case)

    @pl.when(middle >= 10)
    def _():
        run(tile_case)

    copies = [pltpu.make_async_copy(buf, out_ref.at[i], sems.at[i]) for i in range(2)]
    for copy in copies:
        copy.start()
    for copy in copies:
        copy.wait()


def regroup(subsystem, state_real, state_imag):
    half = 64 * 4 * PARTS
    return pl.pallas_call(
        regroup_kernel,
        out_shape=jax.ShapeDtypeStruct((2, half, LANES), jnp.float32),
        in_specs=[
            pl.BlockSpec(memory_space=pltpu.SMEM),
            pl.BlockSpec(memory_space=pltpu.VMEM),
            pl.BlockSpec(memory_space=pltpu.VMEM),
        ],
        out_specs=pl.BlockSpec(memory_space=pl.ANY),
        scratch_shapes=[pltpu.VMEM((half, LANES), jnp.float32), pltpu.SemaphoreType.DMA((2,))],
        name="regroup",
    )(subsystem, state_real.reshape(ROWS, LANES), state_imag.reshape(ROWS, LANES))


def split(value):
    high = value.astype(jnp.bfloat16)
    low = (value - high.astype(jnp.float32)).astype(jnp.bfloat16)
    return high, low


def gram_kernel(place_ref, left_own, left_other, right_own, right_other, out_ref, left):
    def rows(ref, array, index):
        return [
            ref[index + (slice(None), slice(array * 16 + u * 8, array * 16 + u * 8 + 8))].reshape(-1, LANES)
            for u in range(2)
        ]

    @pl.when(pl.program_id(0) == 0)
    def _():
        for half, ref in enumerate((left_own, left_other)):
            re = jnp.concatenate([v for v in rows(ref.at[0, :, 0], 0, ())], axis=1)
            im = jnp.concatenate([v for v in rows(ref.at[0, :, 0], 1, ())], axis=1)
            re_h, re_l = split(re)
            im_h, im_l = split(im)
            blocks = ((re_h, im_h), (re_h, im_h), (re_l, im_l), (im_h, -re_h), (im_h, -re_h), (im_l, -re_l))
            for j, (top, bottom) in enumerate(blocks):
                at = (half * 6 + j) * 256
                left[0:256, at : at + 256] = top
                left[256:512, at : at + 256] = bottom

    right = []
    for ref in (right_own, right_other):
        re_h, re_l = split(jnp.concatenate(rows(ref, 0, ()), axis=1))
        im_h, im_l = split(jnp.concatenate(rows(ref, 1, ()), axis=1))
        right += [re_h, re_l, re_h, im_h, im_l, im_h]
    result = lax.dot_general(
        left[...],
        jnp.concatenate(right, axis=1),
        (((1,), (1,)), ((), ())),
        preferred_element_type=jnp.float32,
    )
    out_ref[:, 0] = result[0:256].reshape(32, 8, 256)
    out_ref[:, 1] = result[256:512].reshape(32, 8, 256)


def gram(place, own, other):
    left_spec = pl.BlockSpec((1, 32, 1, 32, LANES), lambda i, place: (place[0], 0, place[1], 0, 0))
    right_spec = pl.BlockSpec((32, 32, LANES), lambda i, place: (i, 0, 0))
    own5, other5 = (v.reshape(2, 32, 2, 32, LANES) for v in (own, other))
    return pl.pallas_call(
        gram_kernel,
        out_shape=jax.ShapeDtypeStruct((32, 2, 8, 1024), jnp.float32),
        grid_spec=pltpu.PrefetchScalarGridSpec(
            num_scalar_prefetch=1,
            grid=(4,),
            in_specs=[left_spec, left_spec, right_spec, right_spec],
            out_specs=pl.BlockSpec((32, 2, 8, 256), lambda i, place: (0, 0, 0, i)),
            scratch_shapes=[pltpu.VMEM((512, 12 * 256), jnp.bfloat16)],
        ),
        compiler_params=pltpu.CompilerParams(dimension_semantics=("arbitrary",)),
        name="gram",
    )(place, own5, other5, own, other)


def local(state_real, state_imag, subsystem):
    sent = regroup(subsystem, state_real, state_imag).reshape(128, 32, LANES)
    own = lax.all_to_all(sent, DEV, 0, 0, tiled=True)
    other = lax.ppermute(own, "c", [(0, 1), (1, 0)])
    place = jnp.stack([lax.axis_index("yh"), lax.axis_index("c")]).astype(jnp.int32)
    partial = gram(place, own, other)
    received = lax.all_to_all(partial, PEERS, 0, 0, tiled=True)
    total = jnp.sum(received, axis=0) * (1.0 / 16384)
    return total[0], total[1]


def solution(mesh):
    finer = Mesh(mesh.devices.reshape((2,) * 7), DEV)
    return jax.shard_map(
        local,
        mesh=finer,
        in_specs=(P(DEV), P(DEV), P()),
        out_specs=(P(DEV, None), P(DEV, None)),
        check_vma=False,
    )
```

```python
import jax
import jax.numpy as jnp
from jax import lax
from jax.experimental import pallas as pl
from jax.experimental.pallas import tpu as pltpu
from jax.sharding import Mesh
from jax.sharding import PartitionSpec as P

DEV = ("yh", "yl", "zh", "zl", "xh", "xl", "c")
PEERS = ("yl", "zh", "zl", "xh", "xl")
LANES = 128
ROWS = 1024
PARTS = 8
HALF = 64 * 4 * PARTS


def lane_source(middle, lane):
    low_top = lane >> 6
    rest6 = lane & 63
    plain = low_top | (rest6 << 1)
    m = jnp.clip(middle, 1, 6)
    rest5 = lane & 31
    below = rest5 & ((1 << (m - 1)) - 1)
    above = rest5 >> (m - 1)
    both = low_top | (below << 1) | (((lane >> 5) & 1) << m) | (above << (m + 1))
    return jnp.where(middle < 7, both, plain)


def sublane_source(middle, sub):
    m = jnp.clip(middle - 7, 0, 2)
    rest = sub & 3
    below = rest & ((1 << m) - 1)
    above = rest >> m
    return below | ((sub >> 2) << m) | (above << (m + 1))


def regroup_kernel(sub_ref, re_hbm, im_hbm, out_ref, re_ref, im_ref, tall, sems):
    copies = [
        pltpu.make_async_copy(src, dst, sems.at[i])
        for i, (src, dst) in enumerate(((re_hbm, re_ref), (im_hbm, im_ref)))
    ]
    for copy in copies:
        copy.start()
    middle = sub_ref[1]
    lane = lax.broadcasted_iota(jnp.int32, (8, LANES), 1)
    sub = lax.broadcasted_iota(jnp.int32, (8, LANES), 0)
    lane_index = lane_source(middle, lane)
    sub_index = sublane_source(middle, sub)
    low64 = lane < 64
    low32 = (lane & 32) == 0
    low4 = sub < 4

    def load(ref, tile):
        return ref[pl.ds(pl.multiple_of(tile * 8, 8), 8), :]

    def lanes(value):
        return jnp.take_along_axis(value, lane_index, axis=1)

    def swap64(a, b):
        return (
            jnp.where(low64, a, pltpu.roll(b, 64, 1)),
            jnp.where(low64, pltpu.roll(a, 64, 1), b),
        )

    def swap32(a, b):
        return (
            jnp.where(low32, a, pltpu.roll(b, 32, 1)),
            jnp.where(low32, pltpu.roll(a, 96, 1), b),
        )

    def swap_sub(a, b):
        return (
            jnp.where(low4, a, pltpu.roll(b, 4, 0)),
            jnp.where(low4, pltpu.roll(a, 4, 0), b),
        )

    def lane_case(ref, top, k4):
        base = top * 64 + k4 * 4
        a = [lanes(load(ref, base + r)) for r in range(4)]
        b00, b10 = swap64(a[0], a[2])
        b01, b11 = swap64(a[1], a[3])
        return (*swap32(b00, b01), *swap32(b10, b11))

    def sub_case(ref, top, k4):
        base = top * 64 + k4 * 4
        a = [jnp.take_along_axis(lanes(load(ref, base + r)), sub_index, axis=0) for r in range(4)]
        b00, b10 = swap64(a[0], a[2])
        b01, b11 = swap64(a[1], a[3])
        return (*swap_sub(b00, b01), *swap_sub(b10, b11))

    def tile_case(ref, top, k4):
        m = jnp.clip(middle - 10, 0, 5)
        out = []
        for bit in range(2):
            pair = []
            for r in range(2):
                rest = k4 * 2 + r
                below = rest & ((1 << m) - 1)
                above = rest >> m
                tile = top * 64 + (below | (bit << m) | (above << (m + 1)))
                pair.append(lanes(load(ref, tile)))
            out.append(swap64(*pair))
        return (out[0][0], out[1][0], out[0][1], out[1][1])

    def run(case, array, ref):
        def step(k4, carry):
            for top in range(2):
                for which, tile in enumerate(case(ref, top, k4)):
                    part = (which >> 1) + 2 * (which & 1) + 4 * top
                    tall[pl.ds((array * 16 + k4) * 72 + part * 9, 8), :] = tile
            return carry

        lax.fori_loop(0, 16, step, 0, unroll=4)

    for array, ref in enumerate((re_ref, im_ref)):
        copies[array].wait()

        @pl.when(middle < 7)
        def _():
            run(lane_case, array, ref)

        @pl.when((middle >= 7) & (middle < 10))
        def _():
            run(sub_case, array, ref)

        @pl.when(middle >= 10)
        def _():
            run(tile_case, array, ref)

    def finish(k4, carry):
        for array in range(2):
            for sub in range(8):
                tile = tall[pl.ds((array * 16 + k4) * 72 + sub, 8, stride=9), :]
                row = pl.multiple_of(sub * 256 + (k4 >> 1) * 32 + array * 16 + (k4 & 1) * 8, 8)
                out_ref[pl.ds(row, 8), :] = tile
                out_ref[pl.ds(row + HALF, 8), :] = tile
        return carry

    lax.fori_loop(0, 16, finish, 0, unroll=2)


def regroup(subsystem, state_real, state_imag):
    hbm = pl.BlockSpec(memory_space=pl.ANY)
    return pl.pallas_call(
        regroup_kernel,
        out_shape=pltpu.VMEM((2 * HALF, LANES), jnp.float32),
        in_specs=[pl.BlockSpec(memory_space=pltpu.SMEM), hbm, hbm],
        out_specs=pl.BlockSpec(memory_space=pltpu.VMEM),
        scratch_shapes=[
            pltpu.VMEM((ROWS, LANES), jnp.float32),
            pltpu.VMEM((ROWS, LANES), jnp.float32),
            pltpu.VMEM((2 * 16 * 72, LANES), jnp.float32),
            pltpu.SemaphoreType.DMA((2,)),
        ],
        compiler_params=pltpu.CompilerParams(vmem_limit_bytes=8 << 20),
        name="regroup",
    )(
        *(
            pltpu.with_memory_space_constraint(v, pltpu.HBM)
            for v in (subsystem, state_real.reshape(ROWS, LANES), state_imag.reshape(ROWS, LANES))
        )
    )


def split(value):
    high = value.astype(jnp.bfloat16)
    low = (value - high.astype(jnp.float32)).astype(jnp.bfloat16)
    return high, low


def gram_kernel(place_ref, given, *rest):
    added, out_ref = rest if len(rest) == 2 else (None, rest[0])

    def columns(ref, array):
        return split(
            jnp.concatenate(
                [ref[:, array * 16 + u * 8 : array * 16 + u * 8 + 8].reshape(-1, LANES) for u in range(2)],
                axis=1,
            )
        )

    mine = given.at[place_ref[0], :, place_ref[1]]
    re_h, re_l = columns(mine, 0)
    im_h, im_l = columns(mine, 1)
    top = [re_h, re_h, re_l, im_h, im_h, im_l]
    bottom = [im_h, im_h, im_l, -re_h, -re_h, -re_l]
    left = jnp.concatenate([jnp.concatenate(top, axis=1), jnp.concatenate(bottom, axis=1)], axis=0)
    flat = given.reshape(128, 32, LANES)
    for n in range(4):
        cut = flat.at[pl.ds(n * 32, 32)]
        re_h, re_l = columns(cut, 0)
        im_h, im_l = columns(cut, 1)
        result = lax.dot_general(
            left,
            jnp.concatenate([re_h, re_l, re_h, im_h, im_l, im_h], axis=1),
            (((1,), (1,)), ((), ())),
            preferred_element_type=jnp.float32,
        )
        at = slice(n * 256, n * 256 + 256)
        for array in range(2):
            part = result[array * 256 : array * 256 + 256].reshape(32, 8, 256)
            out_ref[:, array, :, at] = part if added is None else (part + added[:, array, :, at]) * (1.0 / 16384)


def gram(place, given, added=None):
    vmem = pl.BlockSpec(memory_space=pltpu.VMEM)
    extra = () if added is None else (added,)
    flops = 2 * 512 * 1024 * 6 * 256
    return pl.pallas_call(
        gram_kernel,
        out_shape=pltpu.VMEM((32, 2, 8, 1024), jnp.float32),
        in_specs=[pl.BlockSpec(memory_space=pltpu.SMEM), vmem, *(vmem for _ in extra)],
        out_specs=vmem,
        input_output_aliases={2: 0} if extra else {},
        compiler_params=pltpu.CompilerParams(vmem_limit_bytes=24 << 20),
        cost_estimate=pl.CostEstimate(flops=flops, transcendentals=0, bytes_accessed=4 << 20),
        name=f"gram{len(extra)}",
    )(place, given.reshape(2, 32, 2, 32, LANES), *extra)


def local(state_real, state_imag, subsystem):
    sent = regroup(subsystem, state_real, state_imag).reshape(128, 32, LANES)
    own = lax.all_to_all(sent, DEV, 0, 0, tiled=True)
    other = lax.ppermute(own, "c", [(0, 1), (1, 0)])
    place = jnp.stack([lax.axis_index("yh"), lax.axis_index("c")]).astype(jnp.int32)
    partial = gram(place, other, gram(place, own))
    received = lax.all_to_all(partial, PEERS, 0, 0, tiled=True)
    return jnp.sum(received[:, 0], axis=0), jnp.sum(received[:, 1], axis=0)


def solution(mesh):
    finer = Mesh(mesh.devices.reshape((2,) * 7), DEV)
    return jax.shard_map(
        local,
        mesh=finer,
        in_specs=(P(DEV), P(DEV), P()),
        out_specs=(P(DEV, None), P(DEV, None)),
        check_vma=False,
    )
```

```python
import jax
import jax.numpy as jnp
from jax import lax
from jax.experimental import pallas as pl
from jax.experimental.pallas import tpu as pltpu
from jax.sharding import Mesh
from jax.sharding import PartitionSpec as P

DEV = ("yh", "yl", "zh", "zl", "xh", "xl", "c")
PEERS = ("yl", "zh", "zl", "xh", "xl")
LANES = 128
ROWS = 1024
PARTS = 8
TERMS = 2
HALF = 64 * 4 * PARTS


def mixing_source(middle, column):
    quad, lane = column >> 7, column & 127
    low, other = quad >> 1, quad & 1
    m = jnp.clip(middle, 1, 6)
    rest5 = lane & 31
    below = rest5 & ((1 << (m - 1)) - 1)
    above = rest5 >> (m - 1)
    both = ((lane >> 5) << 7) | low | (below << 1) | (other << m) | (above << (m + 1))
    plain = (other << 8) | ((lane >> 6) << 7) | low | ((lane & 63) << 1)
    return jnp.where(middle < 7, both, plain)


def sublane_source(middle, sub):
    m = jnp.clip(middle - 7, 0, 2)
    rest = sub & 3
    below = rest & ((1 << m) - 1)
    above = rest >> m
    return below | ((sub >> 2) << m) | (above << (m + 1))


def regroup_kernel(sub_ref, re_hbm, im_hbm, out_ref, re_ref, im_ref, terms, tall, sems):
    copies = [
        pltpu.make_async_copy(src, dst, sems.at[i])
        for i, (src, dst) in enumerate(((re_hbm, re_ref), (im_hbm, im_ref)))
    ]
    for copy in copies:
        copy.start()
    middle = sub_ref[1]
    source = mixing_source(middle, lax.broadcasted_iota(jnp.int32, (16, 512), 1))
    source = source - lax.broadcasted_iota(jnp.int32, (16, 512), 0)
    mixing = jnp.concatenate(
        [jnp.where(source == 16 * i, 1.0, 0.0).astype(jnp.bfloat16) for i in range(32)], axis=0
    )
    place = jnp.where(middle >= 10, middle - 10, 1)

    def load(ref, top, k4, r):
        rest = k4 * 2 + (r & 1)
        below = rest & ((1 << place) - 1)
        tile = top * 64 + (below | ((r >> 1) << place) | ((rest >> place) << (place + 1)))
        return ref[pl.ds(pl.multiple_of(tile * 8, 8), 8), :]

    for array, ref in enumerate((re_ref, im_ref)):
        copies[array].wait()

        def fill(i, carry):
            for top in range(2):
                row = pl.multiple_of(top * 128 + i * 16, 16)
                for r in range(4):
                    value = jnp.concatenate([load(ref, top, 2 * i + j, r) for j in range(2)], axis=0)
                    for t in range(TERMS):
                        term = value.astype(jnp.bfloat16)
                        terms[pl.ds(array * 256 + row, 16), t * 512 + r * 128 : t * 512 + r * 128 + 128] = term
                        value = value - term.astype(jnp.float32)
            return carry

        lax.fori_loop(0, 8, fill, 0, unroll=8)

    mixed = lax.dot_general(
        terms[...],
        jnp.concatenate([mixing] * TERMS, axis=0),
        (((1,), (0,)), ((), ())),
        preferred_element_type=jnp.float32,
    )
    for array in range(2):
        for top in range(2):
            for k4 in range(16):
                row = array * 256 + top * 128 + k4 * 8
                for quad in range(4):
                    part = (quad >> 1) + 2 * (quad & 1) + 4 * top
                    at = (array * 16 + k4) * 72 + part * 9
                    tall[at : at + 8, :] = mixed[row : row + 8, quad * 128 : quad * 128 + 128]

    @pl.when((middle >= 7) & (middle < 10))
    def _():
        sub = lax.broadcasted_iota(jnp.int32, (8, LANES), 0)
        sub_index = sublane_source(middle, sub)
        low4 = sub < 4

        def swap(group, carry):
            for part in (0, 1, 4, 5):
                at = [pl.ds(group * 72 + p * 9, 8) for p in (part, part + 2)]
                a, b = (jnp.take_along_axis(tall[rows, :], sub_index, axis=0) for rows in at)
                tall[at[0], :] = jnp.where(low4, a, pltpu.roll(b, 4, 0))
                tall[at[1], :] = jnp.where(low4, pltpu.roll(a, 4, 0), b)
            return carry

        lax.fori_loop(0, 32, swap, 0, unroll=8)

    for array in range(2):
        def finish(k4, carry):
            for sub in range(8):
                tile = tall[pl.ds((array * 16 + k4) * 72 + sub, 8, stride=9), :]
                row = pl.multiple_of(sub * 256 + (k4 >> 1) * 32 + array * 16 + (k4 & 1) * 8, 8)
                out_ref[pl.ds(row, 8), :] = tile
                out_ref[pl.ds(row + HALF, 8), :] = tile
            return carry

        lax.fori_loop(0, 16, finish, 0, unroll=16)


def regroup(subsystem, state_real, state_imag):
    hbm = pl.BlockSpec(memory_space=pl.ANY)
    return pl.pallas_call(
        regroup_kernel,
        out_shape=pltpu.VMEM((2 * HALF, LANES), jnp.float32),
        in_specs=[pl.BlockSpec(memory_space=pltpu.SMEM), hbm, hbm],
        out_specs=pl.BlockSpec(memory_space=pltpu.VMEM),
        scratch_shapes=[
            pltpu.VMEM((ROWS, LANES), jnp.float32),
            pltpu.VMEM((ROWS, LANES), jnp.float32),
            pltpu.VMEM((512, TERMS * 512), jnp.bfloat16),
            pltpu.VMEM((2 * 16 * 72, LANES), jnp.float32),
            pltpu.SemaphoreType.DMA((2,)),
        ],
        compiler_params=pltpu.CompilerParams(vmem_limit_bytes=12 << 20),
        name="regroup",
    )(
        *(
            pltpu.with_memory_space_constraint(v, pltpu.HBM)
            for v in (subsystem, state_real.reshape(ROWS, LANES), state_imag.reshape(ROWS, LANES))
        )
    )


def split(value):
    high = value.astype(jnp.bfloat16)
    low = (value - high.astype(jnp.float32)).astype(jnp.bfloat16)
    return high, low


def gram_kernel(place_ref, given, *rest):
    added, out_ref = rest if len(rest) == 2 else (None, rest[0])

    def columns(ref, array):
        return split(
            jnp.concatenate(
                [ref[:, array * 16 + u * 8 : array * 16 + u * 8 + 8].reshape(-1, LANES) for u in range(2)],
                axis=1,
            )
        )

    mine = given.at[place_ref[0], :, place_ref[1]]
    re_h, re_l = columns(mine, 0)
    im_h, im_l = columns(mine, 1)
    top = [re_h, re_h, re_l, im_h, im_h, im_l]
    bottom = [im_h, im_h, im_l, -re_h, -re_h, -re_l]
    left = jnp.concatenate([jnp.concatenate(top, axis=1), jnp.concatenate(bottom, axis=1)], axis=0)
    flat = given.reshape(128, 32, LANES)
    for n in range(4):
        cut = flat.at[pl.ds(n * 32, 32)]
        re_h, re_l = columns(cut, 0)
        im_h, im_l = columns(cut, 1)
        result = lax.dot_general(
            left,
            jnp.concatenate([re_h, re_l, re_h, im_h, im_l, im_h], axis=1),
            (((1,), (1,)), ((), ())),
            preferred_element_type=jnp.float32,
        )
        at = slice(n * 256, n * 256 + 256)
        for array in range(2):
            part = result[array * 256 : array * 256 + 256].reshape(32, 8, 256)
            out_ref[:, array, :, at] = part if added is None else (part + added[:, array, :, at]) * (1.0 / 16384)


def gram(place, given, added=None):
    vmem = pl.BlockSpec(memory_space=pltpu.VMEM)
    extra = () if added is None else (added,)
    flops = 2 * 512 * 1024 * 6 * 256
    return pl.pallas_call(
        gram_kernel,
        out_shape=pltpu.VMEM((32, 2, 8, 1024), jnp.float32),
        in_specs=[pl.BlockSpec(memory_space=pltpu.SMEM), vmem, *(vmem for _ in extra)],
        out_specs=vmem,
        input_output_aliases={2: 0} if extra else {},
        compiler_params=pltpu.CompilerParams(vmem_limit_bytes=24 << 20),
        cost_estimate=pl.CostEstimate(flops=flops, transcendentals=0, bytes_accessed=4 << 20),
        name=f"gram{len(extra)}",
    )(place, given.reshape(2, 32, 2, 32, LANES), *extra)


def local(state_real, state_imag, subsystem):
    sent = regroup(subsystem, state_real, state_imag).reshape(128, 32, LANES)
    own = lax.all_to_all(sent, DEV, 0, 0, tiled=True)
    other = lax.ppermute(own, "c", [(0, 1), (1, 0)])
    place = jnp.stack([lax.axis_index("yh"), lax.axis_index("c")]).astype(jnp.int32)
    partial = gram(place, other, gram(place, own))
    received = lax.all_to_all(partial, PEERS, 0, 0, tiled=True)
    return jnp.sum(received[:, 0], axis=0), jnp.sum(received[:, 1], axis=0)


def solution(mesh):
    finer = Mesh(mesh.devices.reshape((2,) * 7), DEV)
    return jax.shard_map(
        local,
        mesh=finer,
        in_specs=(P(DEV), P(DEV), P()),
        out_specs=(P(DEV, None), P(DEV, None)),
        check_vma=False,
    )
```

```python
import jax
import jax.numpy as jnp
from jax import lax
from jax.experimental import pallas as pl
from jax.experimental.pallas import tpu as pltpu
from jax.sharding import Mesh
from jax.sharding import PartitionSpec as P

DEV = ("yh", "yl", "zh", "zl", "xh", "xl", "c")
PEERS = ("yl", "zh", "zl", "xh", "xl")
LANES = 128
ROWS = 1024
PARTS = 8
TERMS = 2
HALF = 64 * 4 * PARTS


def mixing_source(middle, column):
    quad, lane = column >> 7, column & 127
    low, other = quad >> 1, quad & 1
    m = jnp.clip(middle, 1, 6)
    rest5 = lane & 31
    below = rest5 & ((1 << (m - 1)) - 1)
    above = rest5 >> (m - 1)
    both = ((lane >> 5) << 7) | low | (below << 1) | (other << m) | (above << (m + 1))
    plain = (other << 8) | ((lane >> 6) << 7) | low | ((lane & 63) << 1)
    return jnp.where(middle < 7, both, plain)


def sublane_source(middle, sub):
    m = jnp.clip(middle - 7, 0, 2)
    rest = sub & 3
    below = rest & ((1 << m) - 1)
    above = rest >> m
    return below | ((sub >> 2) << m) | (above << (m + 1))


def regroup_kernel(sub_ref, re_hbm, im_hbm, out_ref, re_ref, im_ref, terms, tall, sems):
    copies = [
        pltpu.make_async_copy(src, dst, sems.at[i])
        for i, (src, dst) in enumerate(((re_hbm, re_ref), (im_hbm, im_ref)))
    ]
    for copy in copies:
        copy.start()
    middle = sub_ref[1]
    source = mixing_source(middle, lax.broadcasted_iota(jnp.int32, (16, 512), 1))
    source = source - lax.broadcasted_iota(jnp.int32, (16, 512), 0)
    mixing = jnp.concatenate(
        [jnp.where(source == 16 * i, 1.0, 0.0).astype(jnp.bfloat16) for i in range(32)], axis=0
    )
    place = jnp.where(middle >= 10, middle - 10, 1)

    def load(ref, top, k4, r):
        rest = k4 * 2 + (r & 1)
        below = rest & ((1 << place) - 1)
        tile = top * 64 + (below | ((r >> 1) << place) | ((rest >> place) << (place + 1)))
        return ref[pl.ds(pl.multiple_of(tile * 8, 8), 8), :]

    for array, ref in enumerate((re_ref, im_ref)):
        copies[array].wait()

        def fill(i, carry):
            for top in range(2):
                row = pl.multiple_of(top * 128 + i * 16, 16)
                for r in range(4):
                    value = jnp.concatenate([load(ref, top, 2 * i + j, r) for j in range(2)], axis=0)
                    for t in range(TERMS):
                        term = value.astype(jnp.bfloat16)
                        terms[pl.ds(array * 256 + row, 16), t * 512 + r * 128 : t * 512 + r * 128 + 128] = term
                        value = value - term.astype(jnp.float32)
            return carry

        lax.fori_loop(0, 8, fill, 0, unroll=8)

    mixed = lax.dot_general(
        terms[...],
        jnp.concatenate([mixing] * TERMS, axis=0),
        (((1,), (0,)), ((), ())),
        preferred_element_type=jnp.float32,
    )
    for array in range(2):
        for top in range(2):
            for k4 in range(16):
                row = array * 256 + top * 128 + k4 * 8
                for quad in range(4):
                    part = (quad >> 1) + 2 * (quad & 1) + 4 * top
                    at = (array * 16 + k4) * 72 + part * 9
                    tall[at : at + 8, :] = mixed[row : row + 8, quad * 128 : quad * 128 + 128]

    @pl.when((middle >= 7) & (middle < 10))
    def _():
        sub = lax.broadcasted_iota(jnp.int32, (8, LANES), 0)
        sub_index = sublane_source(middle, sub)
        low4 = sub < 4

        def swap(group, carry):
            for part in (0, 1, 4, 5):
                at = [pl.ds(group * 72 + p * 9, 8) for p in (part, part + 2)]
                a, b = (jnp.take_along_axis(tall[rows, :], sub_index, axis=0) for rows in at)
                tall[at[0], :] = jnp.where(low4, a, pltpu.roll(b, 4, 0))
                tall[at[1], :] = jnp.where(low4, pltpu.roll(a, 4, 0), b)
            return carry

        lax.fori_loop(0, 32, swap, 0, unroll=8)

    for array in range(2):
        def finish(k4, carry):
            for sub in range(8):
                tile = tall[pl.ds((array * 16 + k4) * 72 + sub, 8, stride=9), :]
                row = pl.multiple_of(sub * 256 + (k4 >> 1) * 32 + array * 16 + (k4 & 1) * 8, 8)
                out_ref[pl.ds(row, 8), :] = tile
                out_ref[pl.ds(row + HALF, 8), :] = tile
            return carry

        lax.fori_loop(0, 16, finish, 0, unroll=16)


def regroup(subsystem, state_real, state_imag):
    hbm = pl.BlockSpec(memory_space=pl.ANY)
    return pl.pallas_call(
        regroup_kernel,
        out_shape=pltpu.VMEM((2 * HALF, LANES), jnp.float32),
        in_specs=[pl.BlockSpec(memory_space=pltpu.SMEM), hbm, hbm],
        out_specs=pl.BlockSpec(memory_space=pltpu.VMEM),
        scratch_shapes=[
            pltpu.VMEM((ROWS, LANES), jnp.float32),
            pltpu.VMEM((ROWS, LANES), jnp.float32),
            pltpu.VMEM((512, TERMS * 512), jnp.bfloat16),
            pltpu.VMEM((2 * 16 * 72, LANES), jnp.float32),
            pltpu.SemaphoreType.DMA((2,)),
        ],
        compiler_params=pltpu.CompilerParams(vmem_limit_bytes=12 << 20),
        name="regroup",
    )(
        *(
            pltpu.with_memory_space_constraint(v, pltpu.HBM)
            for v in (subsystem, state_real.reshape(ROWS, LANES), state_imag.reshape(ROWS, LANES))
        )
    )


def split(value):
    high = value.astype(jnp.bfloat16)
    low = (value - high.astype(jnp.float32)).astype(jnp.bfloat16)
    return high, low


def gram_kernel(place_ref, given, *rest):
    added, out_ref = rest if len(rest) == 2 else (None, rest[0])

    def columns(ref, array):
        return split(
            jnp.concatenate(
                [ref[:, array * 16 + u * 8 : array * 16 + u * 8 + 8].reshape(-1, LANES) for u in range(2)],
                axis=1,
            )
        )

    mine = given.at[place_ref[0], :, place_ref[1]]
    re_h, re_l = columns(mine, 0)
    im_h, im_l = columns(mine, 1)
    top = [re_h, re_h, re_l, im_h, im_h, im_l]
    bottom = [im_h, im_h, im_l, -re_h, -re_h, -re_l]
    left = jnp.concatenate([jnp.concatenate(top, axis=1), jnp.concatenate(bottom, axis=1)], axis=0)
    flat = given.reshape(128, 32, LANES)
    for n in range(2):
        cut = flat.at[pl.ds(n * 64, 64)]
        re_h, re_l = columns(cut, 0)
        im_h, im_l = columns(cut, 1)
        result = lax.dot_general(
            left,
            jnp.concatenate([re_h, re_l, re_h, im_h, im_l, im_h], axis=1),
            (((1,), (1,)), ((), ())),
            preferred_element_type=jnp.float32,
        )
        at = slice(n * 512, n * 512 + 512)
        for array in range(2):
            part = result[array * 256 : array * 256 + 256].reshape(32, 8, 512)
            out_ref[:, array, :, at] = part if added is None else (part + added[:, array, :, at]) * (1.0 / 16384)


def gram(place, given, added=None):
    vmem = pl.BlockSpec(memory_space=pltpu.VMEM)
    extra = () if added is None else (added,)
    flops = 2 * 512 * 1024 * 6 * 256
    return pl.pallas_call(
        gram_kernel,
        out_shape=pltpu.VMEM((32, 2, 8, 1024), jnp.float32),
        in_specs=[pl.BlockSpec(memory_space=pltpu.SMEM), vmem, *(vmem for _ in extra)],
        out_specs=vmem,
        input_output_aliases={2: 0} if extra else {},
        compiler_params=pltpu.CompilerParams(vmem_limit_bytes=24 << 20),
        cost_estimate=pl.CostEstimate(flops=flops, transcendentals=0, bytes_accessed=4 << 20),
        name=f"gram{len(extra)}",
    )(place, given.reshape(2, 32, 2, 32, LANES), *extra)


def local(state_real, state_imag, subsystem):
    sent = regroup(subsystem, state_real, state_imag).reshape(128, 32, LANES)
    own = lax.all_to_all(sent, DEV, 0, 0, tiled=True)
    other = lax.ppermute(own, "c", [(0, 1), (1, 0)])
    place = jnp.stack([lax.axis_index("yh"), lax.axis_index("c")]).astype(jnp.int32)
    partial = gram(place, other, gram(place, own))
    received = lax.all_to_all(partial, PEERS, 0, 0, tiled=True)
    return jnp.sum(received[:, 0], axis=0), jnp.sum(received[:, 1], axis=0)


def solution(mesh):
    finer = Mesh(mesh.devices.reshape((2,) * 7), DEV)
    return jax.shard_map(
        local,
        mesh=finer,
        in_specs=(P(DEV), P(DEV), P()),
        out_specs=(P(DEV, None), P(DEV, None)),
        check_vma=False,
    )
```

```python
import jax
import jax.numpy as jnp
from jax import lax
from jax.experimental import pallas as pl
from jax.experimental.pallas import tpu as pltpu
from jax.sharding import Mesh
from jax.sharding import PartitionSpec as P

DEV = ("yh", "yl", "zh", "zl", "xh", "xl", "c")
PEERS = ("yl", "zh", "zl", "xh", "xl")
LANES = 128
ROWS = 1024
PARTS = 8
TERMS = 2
HALF = 64 * 4 * PARTS


def mixing_source(middle, column):
    quad, lane = column >> 7, column & 127
    low, other = quad >> 1, quad & 1
    m = jnp.clip(middle, 1, 6)
    rest5 = lane & 31
    below = rest5 & ((1 << (m - 1)) - 1)
    above = rest5 >> (m - 1)
    both = ((lane >> 5) << 7) | low | (below << 1) | (other << m) | (above << (m + 1))
    plain = (other << 8) | ((lane >> 6) << 7) | low | ((lane & 63) << 1)
    return jnp.where(middle < 7, both, plain)


def sublane_source(middle, sub):
    m = jnp.clip(middle - 7, 0, 2)
    rest = sub & 3
    below = rest & ((1 << m) - 1)
    above = rest >> m
    return below | ((sub >> 2) << m) | (above << (m + 1))


def regroup_kernel(sub_ref, re_hbm, im_hbm, out_ref, re_ref, im_ref, terms, tall, sems):
    copies = [
        pltpu.make_async_copy(src, dst, sems.at[i])
        for i, (src, dst) in enumerate(((re_hbm, re_ref), (im_hbm, im_ref)))
    ]
    for copy in copies:
        copy.start()
    middle = sub_ref[1]
    source = mixing_source(middle, lax.broadcasted_iota(jnp.int32, (16, 512), 1))
    source = source - lax.broadcasted_iota(jnp.int32, (16, 512), 0)
    mixing = jnp.concatenate(
        [jnp.where(source == 16 * i, 1.0, 0.0).astype(jnp.bfloat16) for i in range(32)], axis=0
    )
    place = jnp.where(middle >= 10, middle - 10, 1)

    def load(ref, top, k4, r):
        rest = k4 * 2 + (r & 1)
        below = rest & ((1 << place) - 1)
        tile = top * 64 + (below | ((r >> 1) << place) | ((rest >> place) << (place + 1)))
        return ref[pl.ds(pl.multiple_of(tile * 8, 8), 8), :]

    for array, ref in enumerate((re_ref, im_ref)):
        copies[array].wait()

        def fill(i, carry):
            for top in range(2):
                row = pl.multiple_of(top * 128 + i * 16, 16)
                for r in range(4):
                    value = jnp.concatenate([load(ref, top, 2 * i + j, r) for j in range(2)], axis=0)
                    for t in range(TERMS):
                        term = value.astype(jnp.bfloat16)
                        terms[pl.ds(array * 256 + row, 16), t * 512 + r * 128 : t * 512 + r * 128 + 128] = term
                        value = value - term.astype(jnp.float32)
            return carry

        lax.fori_loop(0, 8, fill, 0, unroll=8)

    mixed = lax.dot_general(
        terms[...],
        jnp.concatenate([mixing] * TERMS, axis=0),
        (((1,), (0,)), ((), ())),
        preferred_element_type=jnp.float32,
    )
    for array in range(2):
        for top in range(2):
            for k4 in range(16):
                row = array * 256 + top * 128 + k4 * 8
                for quad in range(4):
                    part = (quad >> 1) + 2 * (quad & 1) + 4 * top
                    at = (array * 16 + k4) * 72 + part * 9
                    tall[at : at + 8, :] = mixed[row : row + 8, quad * 128 : quad * 128 + 128]

    @pl.when((middle >= 7) & (middle < 10))
    def _():
        sub = lax.broadcasted_iota(jnp.int32, (8, LANES), 0)
        sub_index = sublane_source(middle, sub)
        low4 = sub < 4

        def swap(group, carry):
            for part in (0, 1, 4, 5):
                at = [pl.ds(group * 72 + p * 9, 8) for p in (part, part + 2)]
                a, b = (jnp.take_along_axis(tall[rows, :], sub_index, axis=0) for rows in at)
                tall[at[0], :] = jnp.where(low4, a, pltpu.roll(b, 4, 0))
                tall[at[1], :] = jnp.where(low4, pltpu.roll(a, 4, 0), b)
            return carry

        lax.fori_loop(0, 32, swap, 0, unroll=8)

    for array in range(2):
        def finish(k4, carry):
            for sub in range(8):
                tile = tall[pl.ds((array * 16 + k4) * 72 + sub, 8, stride=9), :]
                row = pl.multiple_of(sub * 256 + (k4 >> 1) * 32 + array * 16 + (k4 & 1) * 8, 8)
                out_ref[pl.ds(row, 8), :] = tile
                out_ref[pl.ds(row + HALF, 8), :] = tile
            return carry

        lax.fori_loop(0, 16, finish, 0, unroll=16)


def regroup(subsystem, state_real, state_imag):
    hbm = pl.BlockSpec(memory_space=pl.ANY)
    return pl.pallas_call(
        regroup_kernel,
        out_shape=pltpu.VMEM((2 * HALF, LANES), jnp.float32),
        in_specs=[pl.BlockSpec(memory_space=pltpu.SMEM), hbm, hbm],
        out_specs=pl.BlockSpec(memory_space=pltpu.VMEM),
        scratch_shapes=[
            pltpu.VMEM((ROWS, LANES), jnp.float32),
            pltpu.VMEM((ROWS, LANES), jnp.float32),
            pltpu.VMEM((512, TERMS * 512), jnp.bfloat16),
            pltpu.VMEM((2 * 16 * 72, LANES), jnp.float32),
            pltpu.SemaphoreType.DMA((2,)),
        ],
        compiler_params=pltpu.CompilerParams(vmem_limit_bytes=12 << 20),
        name="regroup",
    )(
        *(
            pltpu.with_memory_space_constraint(v, pltpu.HBM)
            for v in (subsystem, state_real.reshape(ROWS, LANES), state_imag.reshape(ROWS, LANES))
        )
    )


def split(value):
    high = value.astype(jnp.bfloat16)
    low = (value - high.astype(jnp.float32)).astype(jnp.bfloat16)
    return high, low


def gram_kernel(place_ref, given, *rest):
    added, out_ref = rest if len(rest) == 2 else (None, rest[0])

    def columns(ref, array):
        return split(
            jnp.concatenate(
                [ref[:, array * 16 + u * 8 : array * 16 + u * 8 + 8].reshape(-1, LANES) for u in range(2)],
                axis=1,
            )
        )

    mine = given.at[place_ref[0], :, place_ref[1]]
    re_h, re_l = columns(mine, 0)
    im_h, im_l = columns(mine, 1)
    left = jnp.concatenate(
        [jnp.concatenate([re_h, im_h], axis=1), jnp.concatenate([im_h, -re_h], axis=1)], axis=0
    )
    lower = jnp.concatenate(
        [jnp.concatenate([re_l, im_l], axis=1), jnp.concatenate([im_l, -re_l], axis=1)], axis=0
    )
    tall = jnp.concatenate([left, lower], axis=0)
    flat = given.reshape(128, 32, LANES)
    for n in range(4):
        cut = flat.at[pl.ds(n * 32, 32)]
        re_h, re_l = columns(cut, 0)
        im_h, im_l = columns(cut, 1)
        result = lax.dot_general(
            left,
            jnp.concatenate([re_l, im_l], axis=1),
            (((1,), (1,)), ((), ())),
            preferred_element_type=jnp.float32,
        )
        both = lax.dot_general(
            tall,
            jnp.concatenate([re_h, im_h], axis=1),
            (((1,), (1,)), ((), ())),
            preferred_element_type=jnp.float32,
        )
        result = result + both[0:512] + both[512:1024]
        at = slice(n * 256, n * 256 + 256)
        for array in range(2):
            part = result[array * 256 : array * 256 + 256].reshape(32, 8, 256)
            out_ref[:, array, :, at] = part if added is None else (part + added[:, array, :, at]) * (1.0 / 16384)


def gram(place, given, added=None):
    vmem = pl.BlockSpec(memory_space=pltpu.VMEM)
    extra = () if added is None else (added,)
    flops = 2 * 512 * 1024 * 6 * 256
    return pl.pallas_call(
        gram_kernel,
        out_shape=pltpu.VMEM((32, 2, 8, 1024), jnp.float32),
        in_specs=[pl.BlockSpec(memory_space=pltpu.SMEM), vmem, *(vmem for _ in extra)],
        out_specs=vmem,
        input_output_aliases={2: 0} if extra else {},
        compiler_params=pltpu.CompilerParams(vmem_limit_bytes=24 << 20),
        cost_estimate=pl.CostEstimate(flops=flops, transcendentals=0, bytes_accessed=4 << 20),
        name=f"gram{len(extra)}",
    )(place, given.reshape(2, 32, 2, 32, LANES), *extra)


def local(state_real, state_imag, subsystem):
    sent = regroup(subsystem, state_real, state_imag).reshape(128, 32, LANES)
    own = lax.all_to_all(sent, DEV, 0, 0, tiled=True)
    other = lax.ppermute(own, "c", [(0, 1), (1, 0)])
    place = jnp.stack([lax.axis_index("yh"), lax.axis_index("c")]).astype(jnp.int32)
    partial = gram(place, other, gram(place, own))
    received = lax.all_to_all(partial, PEERS, 0, 0, tiled=True)
    return jnp.sum(received[:, 0], axis=0), jnp.sum(received[:, 1], axis=0)


def solution(mesh):
    finer = Mesh(mesh.devices.reshape((2,) * 7), DEV)
    return jax.shard_map(
        local,
        mesh=finer,
        in_specs=(P(DEV), P(DEV), P()),
        out_specs=(P(DEV, None), P(DEV, None)),
        check_vma=False,
    )
```

```python
import jax
import jax.numpy as jnp
from jax import lax
from jax.experimental import pallas as pl
from jax.experimental.pallas import tpu as pltpu
from jax.sharding import Mesh
from jax.sharding import PartitionSpec as P

DEV = ("yh", "yl", "zh", "zl", "xh", "xl", "c")
PEERS = ("yl", "zh", "zl", "xh", "xl")
LANES = 128
ROWS = 1024
PARTS = 8
TERMS = 2
HALF = 64 * 4 * PARTS


def mixing_source(middle, column):
    quad, lane = column >> 7, column & 127
    low, other = quad >> 1, quad & 1
    m = jnp.clip(middle, 1, 6)
    rest5 = lane & 31
    below = rest5 & ((1 << (m - 1)) - 1)
    above = rest5 >> (m - 1)
    both = ((lane >> 5) << 7) | low | (below << 1) | (other << m) | (above << (m + 1))
    plain = (other << 8) | ((lane >> 6) << 7) | low | ((lane & 63) << 1)
    return jnp.where(middle < 7, both, plain)


def sublane_source(middle, sub):
    m = jnp.clip(middle - 7, 0, 2)
    rest = sub & 3
    below = rest & ((1 << m) - 1)
    above = rest >> m
    return below | ((sub >> 2) << m) | (above << (m + 1))


def regroup_kernel(sub_ref, re_hbm, im_hbm, out_ref, re_ref, im_ref, terms, tall, sems):
    copies = [
        pltpu.make_async_copy(src, dst, sems.at[i])
        for i, (src, dst) in enumerate(((re_hbm, re_ref), (im_hbm, im_ref)))
    ]
    for copy in copies:
        copy.start()
    middle = sub_ref[1]
    source = mixing_source(middle, lax.broadcasted_iota(jnp.int32, (16, 512), 1))
    source = source - lax.broadcasted_iota(jnp.int32, (16, 512), 0)
    mixing = jnp.concatenate(
        [jnp.where(source == 16 * i, 1.0, 0.0).astype(jnp.bfloat16) for i in range(32)], axis=0
    )
    place = jnp.where(middle >= 10, middle - 10, 1)

    def load(ref, top, k4, r):
        rest = k4 * 2 + (r & 1)
        below = rest & ((1 << place) - 1)
        tile = top * 64 + (below | ((r >> 1) << place) | ((rest >> place) << (place + 1)))
        return ref[pl.ds(pl.multiple_of(tile * 8, 8), 8), :]

    for array, ref in enumerate((re_ref, im_ref)):
        copies[array].wait()

        def fill(i, carry):
            for top in range(2):
                row = pl.multiple_of(top * 128 + i * 16, 16)
                for r in range(4):
                    value = jnp.concatenate([load(ref, top, 2 * i + j, r) for j in range(2)], axis=0)
                    for t in range(TERMS):
                        term = value.astype(jnp.bfloat16)
                        terms[pl.ds(t * 512 + array * 256 + row, 16), r * 128 : r * 128 + 128] = term
                        value = value - term.astype(jnp.float32)
            return carry

        lax.fori_loop(0, 8, fill, 0, unroll=8)

    moved = lax.dot_general(terms[...], mixing, (((1,), (0,)), ((), ())), preferred_element_type=jnp.float32)
    mixed = moved[0:512] + moved[512:1024]
    for array in range(2):
        for top in range(2):
            for k4 in range(16):
                row = array * 256 + top * 128 + k4 * 8
                for quad in range(4):
                    part = (quad >> 1) + 2 * (quad & 1) + 4 * top
                    at = (array * 16 + k4) * 72 + part * 9
                    tall[at : at + 8, :] = mixed[row : row + 8, quad * 128 : quad * 128 + 128]

    @pl.when((middle >= 7) & (middle < 10))
    def _():
        sub = lax.broadcasted_iota(jnp.int32, (8, LANES), 0)
        sub_index = sublane_source(middle, sub)
        low4 = sub < 4

        def swap(group, carry):
            for part in (0, 1, 4, 5):
                at = [pl.ds(group * 72 + p * 9, 8) for p in (part, part + 2)]
                a, b = (jnp.take_along_axis(tall[rows, :], sub_index, axis=0) for rows in at)
                tall[at[0], :] = jnp.where(low4, a, pltpu.roll(b, 4, 0))
                tall[at[1], :] = jnp.where(low4, pltpu.roll(a, 4, 0), b)
            return carry

        lax.fori_loop(0, 32, swap, 0, unroll=8)

    for array in range(2):
        def finish(k4, carry):
            for sub in range(8):
                tile = tall[pl.ds((array * 16 + k4) * 72 + sub, 8, stride=9), :]
                row = pl.multiple_of(sub * 256 + (k4 >> 1) * 32 + array * 16 + (k4 & 1) * 8, 8)
                out_ref[pl.ds(row, 8), :] = tile
                out_ref[pl.ds(row + HALF, 8), :] = tile
            return carry

        lax.fori_loop(0, 16, finish, 0, unroll=16)


def regroup(subsystem, state_real, state_imag):
    hbm = pl.BlockSpec(memory_space=pl.ANY)
    return pl.pallas_call(
        regroup_kernel,
        out_shape=pltpu.VMEM((2 * HALF, LANES), jnp.float32),
        in_specs=[pl.BlockSpec(memory_space=pltpu.SMEM), hbm, hbm],
        out_specs=pl.BlockSpec(memory_space=pltpu.VMEM),
        scratch_shapes=[
            pltpu.VMEM((ROWS, LANES), jnp.float32),
            pltpu.VMEM((ROWS, LANES), jnp.float32),
            pltpu.VMEM((TERMS * 512, 512), jnp.bfloat16),
            pltpu.VMEM((2 * 16 * 72, LANES), jnp.float32),
            pltpu.SemaphoreType.DMA((2,)),
        ],
        compiler_params=pltpu.CompilerParams(vmem_limit_bytes=12 << 20),
        name="regroup",
    )(
        *(
            pltpu.with_memory_space_constraint(v, pltpu.HBM)
            for v in (subsystem, state_real.reshape(ROWS, LANES), state_imag.reshape(ROWS, LANES))
        )
    )


def split(value):
    high = value.astype(jnp.bfloat16)
    low = (value - high.astype(jnp.float32)).astype(jnp.bfloat16)
    return high, low


def gram_kernel(place_ref, given, *rest):
    added, out_ref = rest if len(rest) == 2 else (None, rest[0])

    def columns(ref, array):
        return split(
            jnp.concatenate(
                [ref[:, array * 16 + u * 8 : array * 16 + u * 8 + 8].reshape(-1, LANES) for u in range(2)],
                axis=1,
            )
        )

    mine = given.at[place_ref[0], :, place_ref[1]]
    re_h, re_l = columns(mine, 0)
    im_h, im_l = columns(mine, 1)
    top = [re_h, re_h, re_l, im_h, im_h, im_l]
    bottom = [im_h, im_h, im_l, -re_h, -re_h, -re_l]
    left = jnp.concatenate([jnp.concatenate(top, axis=1), jnp.concatenate(bottom, axis=1)], axis=0)
    flat = given.reshape(128, 32, LANES)
    for n in range(4):
        cut = flat.at[pl.ds(n * 32, 32)]
        re_h, re_l = columns(cut, 0)
        im_h, im_l = columns(cut, 1)
        result = lax.dot_general(
            left,
            jnp.concatenate([re_h, re_l, re_h, im_h, im_l, im_h], axis=1),
            (((1,), (1,)), ((), ())),
            preferred_element_type=jnp.float32,
        )
        at = slice(n * 256, n * 256 + 256)
        for array in range(2):
            part = result[array * 256 : array * 256 + 256].reshape(32, 8, 256)
            out_ref[:, array, :, at] = part if added is None else (part + added[:, array, :, at]) * (1.0 / 16384)


def gram(place, given, added=None):
    vmem = pl.BlockSpec(memory_space=pltpu.VMEM)
    extra = () if added is None else (added,)
    flops = 2 * 512 * 1024 * 6 * 256
    return pl.pallas_call(
        gram_kernel,
        out_shape=pltpu.VMEM((32, 2, 8, 1024), jnp.float32),
        in_specs=[pl.BlockSpec(memory_space=pltpu.SMEM), vmem, *(vmem for _ in extra)],
        out_specs=vmem,
        input_output_aliases={2: 0} if extra else {},
        compiler_params=pltpu.CompilerParams(vmem_limit_bytes=24 << 20),
        cost_estimate=pl.CostEstimate(flops=flops, transcendentals=0, bytes_accessed=4 << 20),
        name=f"gram{len(extra)}",
    )(place, given.reshape(2, 32, 2, 32, LANES), *extra)


def local(state_real, state_imag, subsystem):
    sent = regroup(subsystem, state_real, state_imag).reshape(128, 32, LANES)
    own = lax.all_to_all(sent, DEV, 0, 0, tiled=True)
    other = lax.ppermute(own, "c", [(0, 1), (1, 0)])
    place = jnp.stack([lax.axis_index("yh"), lax.axis_index("c")]).astype(jnp.int32)
    partial = gram(place, other, gram(place, own))
    received = lax.all_to_all(partial, PEERS, 0, 0, tiled=True)
    return jnp.sum(received[:, 0], axis=0), jnp.sum(received[:, 1], axis=0)


def solution(mesh):
    finer = Mesh(mesh.devices.reshape((2,) * 7), DEV)
    return jax.shard_map(
        local,
        mesh=finer,
        in_specs=(P(DEV), P(DEV), P()),
        out_specs=(P(DEV, None), P(DEV, None)),
        check_vma=False,
    )
```
